32 devices in a mesh: seq: 8 (over z, core), fsdp: 4 (over y, x).
Axes of the slice: x: 2, y: 2, z: 4, core: 2. Of those that a mesh axis runs over, the one named last changes fastest.
Arguments:
- patches: bfloat16 [4, 1024, 3072], P('fsdp', 'seq'), may hold values from -6 to 6
- weight_codes: int32 [3072, 3072], P('fsdp'), may hold values from -448 to 448
- block_scales: float32 [24, 24], P('fsdp'), may hold values from 2.5e-05 to 0.0001
- key_proj: bfloat16 [4, 1024, 3072], P('fsdp', 'seq'), may hold values from -6 to 6
- value_proj: bfloat16 [4, 1024, 3072], P('fsdp', 'seq'), may hold values from -6 to 6
- query_gain: float32 [3072], replicated, may hold values from 1 to 10
- key_gain: float32 [3072], replicated, may hold values from 1 to 10
Outputs:
- attended: bfloat16 [4, 1024, 3072], P('fsdp', 'seq')
The draws below stay inside these ranges and needn't reach their ends.
All inputs are finite; a program needn't handle non-finite values.
Results may differ from the reference program's by a relative error of at most 0.007.
The reference program's roundings to bfloat16 on the way count: a program that leaves them out, or rounds other values in their place, can miss the bound.
Values may be sent and summed in bfloat16 or wider, within the bound.
A program may use at most 192 MiB of HBM per device.

```python
import math
import jax
import jax.numpy as jnp
from jax import lax

D = 3072
HEADS = 48
HDIM = 64
BLOCK = 128
IMAGES = 4
SEQ = 1024


def gain_values(key, which):
    own_key = jax.random.fold_in(key, which)
    values = jnp.exp(jax.random.uniform(own_key, (HEADS, HDIM), minval=0.0, maxval=math.log(3.0)))
    return values.reshape(HEADS * HDIM).astype(jnp.float32)


def draw_query_gain(key, part):
    return gain_values(key, 1)


def draw_key_gain(key, part):
    return gain_values(key, 2)


def touch_ends(drawn, rng, least, high):
    index_at = [jax.random.randint(jax.random.fold_in(rng, axis), (), 0, length) for axis, length in enumerate(drawn.shape)]
    longest = drawn.shape.index(max(drawn.shape))
    next_to = index_at[:longest] + [(index_at[longest] + 1) % drawn.shape[longest]] + index_at[longest + 1:]
    return drawn.at[tuple(index_at)].set(least).at[tuple(next_to)].set(high)


def block_scale(key, dims, pieces, smallest, high):
    gain, own = 1.0, jax.random.fold_in(key, 6)
    for dim, shards_of in pieces:
        steps = jnp.exp(jax.random.uniform(jax.random.fold_in(own, dim), (shards_of,), jnp.float32, smallest / len(pieces), high / len(pieces)))
        gain = gain * jnp.repeat(steps, dims[dim] // shards_of).reshape([-1 if axis == dim else 1 for axis in range(len(dims))])
    return gain


def bell_draw(key, shape, deviation, limit, shards=(), held_as=jnp.bfloat16):
    values = deviation * jax.random.normal(key, shape, jnp.float32)
    if shards:
        values = values * block_scale(key, shape, shards, -0.22, 0.18)
    return jnp.clip(values, -limit, limit).astype(held_as)


def setup_inputs(seed: int = 0) -> dict:
    keys = jax.random.split(jax.random.key(seed), 8)
    return {
        "patches": bell_draw(keys[0], (IMAGES, SEQ, D), 1.0, 6.0, ((0, 4), (1, 8))),
        "weight_codes": touch_ends(jax.random.randint(keys[1], (D, HEADS * HDIM), -448, 449), jax.random.fold_in(keys[1], 1), -448, 448).astype(jnp.int32),
        "block_scales": jnp.clip(jnp.exp(math.log(0.0001) - 1.3862944 * jax.random.uniform(keys[2], (D // BLOCK, HEADS * HDIM // BLOCK), jnp.float32) ** block_scale(keys[2], (D // BLOCK, HEADS * HDIM // BLOCK), ((0, 4),), -0.2, 0.2)), 2.499999936844688e-05, 0.0001),
        "key_proj": bell_draw(keys[3], (IMAGES, SEQ, HEADS * HDIM), 1.0, 6.0, ((0, 4), (1, 8))),
        "value_proj": bell_draw(keys[4], (IMAGES, SEQ, HEADS * HDIM), 1.0, 6.0, ((0, 4), (1, 8))),
        "query_gain": draw_query_gain(jax.random.fold_in(keys[7], 71), 0),
        "key_gain": draw_key_gain(jax.random.fold_in(keys[7], 71), 0),
    }


NORM_FLOOR = 0.25

def head_norm(projected, gain_row):
    shaped = projected.reshape(projected.shape[:-1] + (HEADS, HDIM))
    average = lax.optimization_barrier(jnp.mean(shaped, axis=-1, keepdims=True))
    centred = shaped - average
    spread = lax.optimization_barrier(jnp.mean(centred * centred, axis=-1, keepdims=True))
    normed = centred * lax.rsqrt(spread + NORM_FLOOR) * gain_row.reshape(HEADS, HDIM)
    return normed.astype(jnp.bfloat16)

def reference(patches, weight_codes, block_scales, key_proj, value_proj, query_gain, key_gain):
    column_count = HEADS * HDIM
    blocked = weight_codes.astype(jnp.float32).reshape(D // BLOCK, BLOCK, column_count // BLOCK, BLOCK)
    weight = (blocked * block_scales[:, None, :, None]).reshape(D, column_count).astype(jnp.bfloat16)
    queries = jnp.dot(patches.reshape(IMAGES * SEQ, D), weight, preferred_element_type=jnp.float32)
    queries = queries.reshape(IMAGES, SEQ, column_count)
    query_view = head_norm(queries, query_gain)
    key_view = head_norm(key_proj.astype(jnp.float32), key_gain)
    value_view = value_proj.reshape(IMAGES, SEQ, HEADS, HDIM)

    def one_head(members):
        query_head, key_head, value_head = members
        scores = jnp.einsum('iqd,ikd->iqk', query_head.astype(jnp.float32), key_head.astype(jnp.float32)) * HDIM ** (-0.5)
        largest = lax.optimization_barrier(jnp.max(scores, axis=-1, keepdims=True))
        probability = jnp.exp(scores - largest)
        normaliser = lax.optimization_barrier(jnp.sum(probability, axis=-1))
        rounded = lax.optimization_barrier(probability.astype(jnp.bfloat16))
        blended = jnp.einsum('iqk,ikd->iqd', rounded.astype(jnp.float32), value_head.astype(jnp.float32))
        return blended / normaliser[..., None]
    outputs = lax.map(one_head, (jnp.moveaxis(query_view, 2, 0), jnp.moveaxis(key_view, 2, 0), jnp.moveaxis(value_view, 2, 0)))
    return jnp.moveaxis(outputs, 0, 2).reshape(IMAGES, SEQ, column_count).astype(jnp.bfloat16)
```

```python
import functools
import math
import jax
import jax.numpy as jnp
from jax import lax
from jax.experimental import pallas as pl
from jax.experimental.pallas import tpu as pltpu
from jax.sharding import PartitionSpec as P

HEADS = 48
HDIM = 64
BLOCK = 128


NORM_FLOOR = 0.25


def head_norm(projected, gain_row):
    shaped = projected.reshape(projected.shape[:-1] + (HEADS, HDIM))
    average = jnp.mean(shaped, axis=-1, keepdims=True)
    centred = shaped - average
    spread = jnp.mean(centred * centred, axis=-1, keepdims=True)
    normed = centred * lax.rsqrt(spread + NORM_FLOOR) * gain_row.reshape(HEADS, HDIM)
    return normed.astype(jnp.bfloat16)


def dequantize(weight_codes, block_scales):
    row_count, column_count = weight_codes.shape
    blocked = weight_codes.astype(jnp.float32).reshape(
        row_count // BLOCK, BLOCK, column_count // BLOCK, BLOCK
    )
    return (
        (blocked * block_scales[:, None, :, None])
        .reshape(row_count, column_count)
        .astype(jnp.bfloat16)
    )


def start_of(query_view):
    image_count, token_count, head_count = (
        query_view.shape[0],
        query_view.shape[1],
        query_view.shape[2],
    )
    return (
        jnp.full((image_count, token_count, head_count), -1e30, jnp.float32),
        jnp.zeros((image_count, token_count, head_count), jnp.float32),
        jnp.zeros(query_view.shape, jnp.float32),
    )


def attend_block(query_view, state_now, key_view, value_view):
    running_max, running_sum, weighted = state_now
    scores = jnp.einsum(
        "ithd,ishd->iths", query_view, key_view, preferred_element_type=jnp.float32
    ) * HDIM ** (-0.5)
    newest = jnp.maximum(running_max, jnp.max(scores, axis=-1))
    probability = jnp.exp(scores - newest[..., None])
    running_sum = jnp.sum(probability, axis=-1)
    blended = jnp.einsum(
        "iths,ishd->ithd",
        probability.astype(jnp.bfloat16),
        value_view,
        preferred_element_type=jnp.float32,
    )
    weighted = blended
    return (newest, running_sum, weighted)


def per_device(patches, weight_codes, block_scales, key_proj, value_proj, query_gain, key_gain):
    image_count, token_count, feature_count = patches.shape
    flat_rows = patches.reshape(image_count * token_count, feature_count)
    key_norm = head_norm(key_proj.astype(jnp.float32), key_gain)
    value_view = value_proj.reshape(image_count, token_count, HEADS, HDIM)
    local_weight = dequantize(weight_codes, block_scales)
    group_rows = lax.all_to_all(flat_rows, "fsdp", split_axis=1, concat_axis=0, tiled=True)
    queries = lax.psum_scatter(
        jnp.dot(group_rows, local_weight, preferred_element_type=jnp.float32),
        "fsdp",
        scatter_dimension=0,
        tiled=True,
    )
    query_view = head_norm(queries, query_gain).reshape(image_count, token_count, HEADS, HDIM)
    finished = attend_block(
        query_view,
        start_of(query_view),
        lax.all_gather(key_norm, "seq", axis=1, tiled=True),
        lax.all_gather(value_view, "seq", axis=1, tiled=True),
    )
    attended = finished[2] / finished[1][..., None]
    return attended.reshape(image_count, token_count, HEADS * HDIM).astype(jnp.bfloat16)


MESH = pl.DeviceIdType.MESH
LANES = 128
CORES = 2


def column_norm(values, gain_row):
    lane = lambda axis: lax.broadcasted_iota(jnp.int32, (LANES, LANES), axis) < HDIM
    spread_out = jnp.where(lane(0) == lane(1), 1.0 / HDIM, 0.0).astype(jnp.float32)
    mean_of = lambda t: jnp.dot(t, spread_out, preferred_element_type=jnp.float32, precision=lax.Precision.HIGHEST)
    centred = values - mean_of(values)
    normed = centred * lax.rsqrt(mean_of(centred * centred) + NORM_FLOOR) * gain_row
    return normed.astype(jnp.bfloat16)


def fused_kernel(
    n, fn, patches, codes, scales, key, value, query_gain, key_gain, out,
    pbuf, cbuf, wbuf, kraw, vbuf, knorm, qsend, qbuf, obuf,
    local_sem, code_sem, p_send, p_recv, fw_send, fw_recv, w_send, w_recv,
    kv_send, kv_recv, q_send, q_recv, o_send, o_recv, own_sem,
):
    s, f = lax.axis_index("seq"), lax.axis_index("fsdp")
    m = n // 2
    half, place = s // m, lax.rem(s, m)
    tokens = patches.shape[0]
    rows, columns = codes.shape
    width = columns // n
    chunks = width // LANES
    group = m * tokens
    chips = m // CORES
    partner = s + 1 - 2 * lax.rem(s, CORES)

    def chip_mate(d):
        return half * m + lax.rem(place + d * CORES, m)

    def rows_of(device):
        return pl.ds(pl.multiple_of(lax.rem(device, m) * tokens, tokens), tokens)

    def all_rows_of(device):
        return pl.ds(pl.multiple_of(device * tokens, tokens), tokens)

    def owned(device):
        return pl.multiple_of((lax.rem(device, m) * 2 + device // m) * width, LANES)

    def chunk_column(q):
        side = jnp.where(q < chunks, 1 - half, half)
        return pl.multiple_of((place * 2 + side) * width + lax.rem(q, chunks) * LANES, LANES)

    code_copies = []
    for q in range(2 * chunks):
        code_copies.append(pltpu.make_async_copy(
            codes.at[:, pl.ds(chunk_column(q), LANES)], cbuf.at[q], code_sem.at[q]))
        code_copies[-1].start()
    own_copies = [
        pltpu.make_async_copy(patches, pbuf.at[rows_of(s)], local_sem.at[0]),
        pltpu.make_async_copy(key.at[:, pl.ds(owned(s), width)], kraw.at[all_rows_of(s)], local_sem.at[1]),
        pltpu.make_async_copy(value.at[:, pl.ds(owned(s), width)], vbuf.at[all_rows_of(s)], local_sem.at[2]),
    ]
    for copy in own_copies:
        copy.start()

    barrier = pltpu.get_barrier_semaphore()
    for d in range(1, n):
        pl.semaphore_signal(barrier, inc=1, device_id={"seq": lax.rem(s + d, n)}, device_id_type=MESH)
    for d in range(1, fn):
        pl.semaphore_signal(barrier, inc=1, device_id={"fsdp": lax.rem(f + d, fn)}, device_id_type=MESH)
    pl.semaphore_wait(barrier, n - 1 + fn - 1)

    def remote(src, dst, send, recv, **device):
        return pltpu.make_async_remote_copy(
            src_ref=src, dst_ref=dst, send_sem=send, recv_sem=recv, device_id=device, device_id_type=MESH)

    patch_copies = [remote(patches, pbuf.at[rows_of(s)], p_send.at[0], p_recv.at[0], seq=partner)]
    for d in range(1, chips):
        patch_copies.append(remote(patches, pbuf.at[rows_of(s)], p_send.at[d], p_recv.at[d], seq=chip_mate(d)))
    for copy in patch_copies[1:] + patch_copies[:1]:
        copy.start()
    kv_copies = []
    for which, (src, dst) in enumerate(((key, kraw), (value, vbuf))):
        for d in range(1, n):
            to = lax.rem(s + d, n)
            kv_copies.append(remote(
                src.at[:, pl.ds(owned(to), width)], dst.at[all_rows_of(s)],
                kv_send.at[which, d], kv_recv.at[which, d], seq=to))
            kv_copies[-1].start()

    own_rows = pl.ds(pl.multiple_of(f * rows, rows), rows)

    def weight_copies(q):
        return [
            remote(wbuf.at[q, own_rows], wbuf.at[q, own_rows], w_send.at[q, d], w_recv.at[q, d],
                   fsdp=lax.rem(f + d, fn))
            for d in range(1, fn)
        ]

    def dequantize_chunk(q, _):
        pltpu.make_async_copy(
            codes.at[:, pl.ds(chunk_column(q), LANES)], cbuf.at[q], code_sem.at[q]).wait()
        for block in range(rows // BLOCK):
            scale = scales[block, chunk_column(q) // BLOCK]
            piece = cbuf[q, block * BLOCK:(block + 1) * BLOCK, :].astype(jnp.float32) * scale
            wbuf[q, pl.ds(pl.multiple_of(f * rows + block * BLOCK, BLOCK), BLOCK), :] = piece.astype(jnp.bfloat16)
        for copy in weight_copies(q):
            copy.start()
        return 0

    lax.fori_loop(0, 2 * chunks, dequantize_chunk, 0)

    own_copies[0].wait()
    forwards = []
    for d in range(1, chips):
        patch_copies[d].wait()
        came_from = half * m + lax.rem(place + m - d * CORES, m)
        forwards.append(remote(
            pbuf.at[rows_of(came_from)], pbuf.at[rows_of(came_from)], fw_send.at[d], fw_recv.at[d], seq=partner))
        forwards[-1].start()
    patch_copies[0].wait()
    for copy in forwards:
        copy.wait()

    def project(q):
        for copy in weight_copies(q):
            copy.wait()
        queries = jnp.dot(pbuf[...], wbuf[q], preferred_element_type=jnp.float32)
        return column_norm(queries, query_gain[:, pl.ds(chunk_column(q), LANES)])

    other = lax.rem(s + m, n)
    half_rows = pl.ds(pl.multiple_of(half * group, group), group)

    def query_copy(k):
        return remote(qsend.at[k], qbuf.at[k, half_rows], q_send.at[k], q_recv.at[k], seq=other)

    def exchange_chunk(k, _):
        qsend[k] = project(k)
        query_copy(k).start()
        return 0

    lax.fori_loop(0, chunks, exchange_chunk, 0)

    own_copies[1].wait()
    own_copies[2].wait()
    for copy in kv_copies:
        copy.wait()

    def key_chunk(k, _):
        at = pl.multiple_of(k * LANES, LANES)
        knorm[k] = column_norm(
            kraw[:, pl.ds(at, LANES)].astype(jnp.float32),
            key_gain[:, pl.ds(pl.multiple_of(owned(s) + at, LANES), LANES)])
        return 0

    lax.fori_loop(0, chunks, key_chunk, 0)

    tile = 2 * tokens
    exponent = HDIM ** (-0.5) * math.log2(math.e)

    def out_columns(k):
        return pl.ds(pl.multiple_of(owned(s) + k * LANES, LANES), LANES)

    def out_copies(k):
        return [
            remote(obuf.at[k, all_rows_of(lax.rem(s + d, n))], out.at[:, out_columns(k)],
                   o_send.at[k, d], o_recv.at[k, d], seq=lax.rem(s + d, n))
            for d in range(1, n)
        ]

    def own_out(k):
        return pltpu.make_async_copy(obuf.at[k, all_rows_of(s)], out.at[:, out_columns(k)], own_sem.at[k])

    def attend_chunk(k, _):
        qbuf[k, half_rows] = project(chunks + k)
        query_copy(k).wait()
        values = vbuf[:, pl.ds(pl.multiple_of(k * LANES, LANES), LANES)]
        keys = knorm[k]
        first = lax.broadcasted_iota(jnp.int32, (tile, LANES), 1) < HDIM

        def attend_tile(i, _):
            here = pl.ds(pl.multiple_of(i * tile, tile), tile)
            queries = qbuf[k, here]
            results = []
            for mine in (first, jnp.logical_not(first)):
                masked = jnp.where(mine, queries, jnp.zeros_like(queries))
                scores = lax.dot_general(
                    masked, keys, (((1,), (1,)), ((), ())), preferred_element_type=jnp.float32)
                largest = jnp.max(scores, axis=-1, keepdims=True)
                probability = jnp.exp2((scores - largest) * exponent)
                normaliser = jnp.sum(probability, axis=-1, keepdims=True)
                blended = jnp.dot(
                    probability.astype(jnp.bfloat16), values, preferred_element_type=jnp.float32)
                results.append(blended / normaliser)
            obuf[k, here] = jnp.where(first, results[0], results[1]).astype(jnp.bfloat16)
            return 0

        lax.fori_loop(0, n * tokens // tile, attend_tile, 0)
        own_out(k).start()
        for copy in out_copies(k):
            copy.start()
        return 0

    lax.fori_loop(0, chunks, attend_chunk, 0)

    def finish(k, _):
        own_out(k).wait()
        for copy in out_copies(k):
            copy.wait()
        return 0

    lax.fori_loop(0, chunks, finish, 0)


def fused_per_device(n, fn, patches, weight_codes, block_scales, key_proj, value_proj, query_gain, key_gain):
    _, tokens, features = patches.shape
    rows, columns = weight_codes.shape
    width = columns // n
    chunks = width // LANES
    group = n // 2 * tokens
    bf16 = jnp.bfloat16
    dma = pltpu.SemaphoreType.DMA
    anywhere = pl.BlockSpec(memory_space=pl.ANY)
    vmem = pl.BlockSpec(memory_space=pltpu.VMEM)
    result = pl.pallas_call(
        functools.partial(fused_kernel, n, fn),
        out_shape=jax.ShapeDtypeStruct((tokens, columns), bf16),
        in_specs=[anywhere, anywhere, pl.BlockSpec(memory_space=pltpu.SMEM), anywhere, anywhere, vmem, vmem],
        out_specs=anywhere,
        scratch_shapes=[
            pltpu.VMEM((group, features), bf16),
            pltpu.VMEM((2 * chunks, rows, LANES), jnp.int32),
            pltpu.VMEM((2 * chunks, features, LANES), bf16),
            pltpu.VMEM((n * tokens, width), bf16),
            pltpu.VMEM((n * tokens, width), bf16),
            pltpu.VMEM((chunks, n * tokens, LANES), bf16),
            pltpu.VMEM((chunks, group, LANES), bf16),
            pltpu.VMEM((chunks, n * tokens, LANES), bf16),
            pltpu.VMEM((chunks, n * tokens, LANES), bf16),
            dma((3,)), dma((2 * chunks,)),
            dma((n,)), dma((n,)), dma((n,)), dma((n,)),
            dma((2 * chunks, fn)), dma((2 * chunks, fn)),
            dma((2, n)), dma((2, n)),
            dma((chunks,)), dma((chunks,)),
            dma((chunks, n)), dma((chunks, n)), dma((chunks,)),
        ],
        compiler_params=pltpu.CompilerParams(
            collective_id=0, has_side_effects=True, vmem_limit_bytes=56 * 1024 * 1024),
    )(
        patches.reshape(tokens, features), weight_codes, block_scales,
        key_proj.reshape(tokens, columns), value_proj.reshape(tokens, columns),
        query_gain.reshape(1, columns), key_gain.reshape(1, columns),
    )
    return result.reshape(1, tokens, columns)


def solution(mesh):
    n, fn = mesh.shape["seq"], mesh.shape["fsdp"]
    specs = (
        P("fsdp", "seq", None), P("fsdp", None), P("fsdp", None),
        P("fsdp", "seq", None), P("fsdp", "seq", None), P(), P(),
    )

    def whole(*arrays):
        patches, weight_codes = arrays[:2]
        fits = patches.shape[0] == fn and weight_codes.shape[1] % (n * LANES) == 0 and n % (2 * CORES) == 0
        body = functools.partial(fused_per_device, n, fn) if fits else per_device
        return jax.shard_map(
            body, mesh=mesh, in_specs=specs, out_specs=P("fsdp", "seq", None), check_vma=False
        )(*arrays)

    return whole
```

```python
import functools
import math
import jax
import jax.numpy as jnp
from jax import lax
from jax.experimental import pallas as pl
from jax.experimental.pallas import tpu as pltpu
from jax.sharding import PartitionSpec as P

HEADS = 48
HDIM = 64
BLOCK = 128


NORM_FLOOR = 0.25


def head_norm(projected, gain_row):
    shaped = projected.reshape(projected.shape[:-1] + (HEADS, HDIM))
    average = jnp.mean(shaped, axis=-1, keepdims=True)
    centred = shaped - average
    spread = jnp.mean(centred * centred, axis=-1, keepdims=True)
    normed = centred * lax.rsqrt(spread + NORM_FLOOR) * gain_row.reshape(HEADS, HDIM)
    return normed.astype(jnp.bfloat16)


def dequantize(weight_codes, block_scales):
    row_count, column_count = weight_codes.shape
    blocked = weight_codes.astype(jnp.float32).reshape(
        row_count // BLOCK, BLOCK, column_count // BLOCK, BLOCK
    )
    return (
        (blocked * block_scales[:, None, :, None])
        .reshape(row_count, column_count)
        .astype(jnp.bfloat16)
    )


def start_of(query_view):
    image_count, token_count, head_count = (
        query_view.shape[0],
        query_view.shape[1],
        query_view.shape[2],
    )
    return (
        jnp.full((image_count, token_count, head_count), -1e30, jnp.float32),
        jnp.zeros((image_count, token_count, head_count), jnp.float32),
        jnp.zeros(query_view.shape, jnp.float32),
    )


def attend_block(query_view, state_now, key_view, value_view):
    running_max, running_sum, weighted = state_now
    scores = jnp.einsum(
        "ithd,ishd->iths", query_view, key_view, preferred_element_type=jnp.float32
    ) * HDIM ** (-0.5)
    newest = jnp.maximum(running_max, jnp.max(scores, axis=-1))
    probability = jnp.exp(scores - newest[..., None])
    running_sum = jnp.sum(probability, axis=-1)
    blended = jnp.einsum(
        "iths,ishd->ithd",
        probability.astype(jnp.bfloat16),
        value_view,
        preferred_element_type=jnp.float32,
    )
    weighted = blended
    return (newest, running_sum, weighted)


def per_device(patches, weight_codes, block_scales, key_proj, value_proj, query_gain, key_gain):
    image_count, token_count, feature_count = patches.shape
    flat_rows = patches.reshape(image_count * token_count, feature_count)
    key_norm = head_norm(key_proj.astype(jnp.float32), key_gain)
    value_view = value_proj.reshape(image_count, token_count, HEADS, HDIM)
    local_weight = dequantize(weight_codes, block_scales)
    group_rows = lax.all_to_all(flat_rows, "fsdp", split_axis=1, concat_axis=0, tiled=True)
    queries = lax.psum_scatter(
        jnp.dot(group_rows, local_weight, preferred_element_type=jnp.float32),
        "fsdp",
        scatter_dimension=0,
        tiled=True,
    )
    query_view = head_norm(queries, query_gain).reshape(image_count, token_count, HEADS, HDIM)
    finished = attend_block(
        query_view,
        start_of(query_view),
        lax.all_gather(key_norm, "seq", axis=1, tiled=True),
        lax.all_gather(value_view, "seq", axis=1, tiled=True),
    )
    attended = finished[2] / finished[1][..., None]
    return attended.reshape(image_count, token_count, HEADS * HDIM).astype(jnp.bfloat16)


MESH = pl.DeviceIdType.MESH
LANES = 128
CORES = 2


def column_norm(values, gain_row):
    lane = lambda axis: lax.broadcasted_iota(jnp.int32, (LANES, LANES), axis) < HDIM
    spread_out = jnp.where(lane(0) == lane(1), 1.0 / HDIM, 0.0).astype(jnp.bfloat16)
    spread_out = jnp.concatenate([spread_out, spread_out], axis=0)

    def mean_of(t):
        high = t.astype(jnp.bfloat16)
        low = (t - high.astype(jnp.float32)).astype(jnp.bfloat16)
        return jnp.dot(jnp.concatenate([high, low], axis=1), spread_out, preferred_element_type=jnp.float32)

    centred = values - mean_of(values)
    normed = centred * lax.rsqrt(mean_of(centred * centred) + NORM_FLOOR) * gain_row
    return normed.astype(jnp.bfloat16)


def fused_kernel(
    n, fn, patches, codes, scales, key, value, query_gain, key_gain, out,
    pbuf, cbuf, wbuf, kraw, vbuf, knorm, qsend, qbuf, obuf,
    local_sem, code_sem, p_send, p_recv, fw_send, fw_recv, w_send, w_recv,
    kv_send, kv_recv, q_send, q_recv, o_send, o_recv, own_sem,
):
    s, f = lax.axis_index("seq"), lax.axis_index("fsdp")
    m = n // 2
    half, place = s // m, lax.rem(s, m)
    tokens = patches.shape[0]
    rows, columns = codes.shape
    width = columns // n
    chunks = width // LANES
    group = m * tokens
    chips = m // CORES
    partner = s + 1 - 2 * lax.rem(s, CORES)

    def chip_mate(d):
        return half * m + lax.rem(place + d * CORES, m)

    def rows_of(device):
        return pl.ds(pl.multiple_of(lax.rem(device, m) * tokens, tokens), tokens)

    def all_rows_of(device):
        return pl.ds(pl.multiple_of(device * tokens, tokens), tokens)

    def owned(device):
        return pl.multiple_of((lax.rem(device, m) * 2 + device // m) * width, LANES)

    def chunk_column(q):
        side = jnp.where(q < chunks, 1 - half, half)
        return pl.multiple_of((place * 2 + side) * width + lax.rem(q, chunks) * LANES, LANES)

    code_copies = []
    for q in range(2 * chunks):
        code_copies.append(pltpu.make_async_copy(
            codes.at[:, pl.ds(chunk_column(q), LANES)], cbuf.at[q], code_sem.at[q]))
        code_copies[-1].start()
    own_copies = [
        pltpu.make_async_copy(patches, pbuf.at[rows_of(s)], local_sem.at[0]),
        pltpu.make_async_copy(key.at[:, pl.ds(owned(s), width)], kraw.at[all_rows_of(s)], local_sem.at[1]),
        pltpu.make_async_copy(value.at[:, pl.ds(owned(s), width)], vbuf.at[all_rows_of(s)], local_sem.at[2]),
    ]
    for copy in own_copies:
        copy.start()

    barrier = pltpu.get_barrier_semaphore()
    for d in range(1, n):
        pl.semaphore_signal(barrier, inc=1, device_id={"seq": lax.rem(s + d, n)}, device_id_type=MESH)
    for d in range(1, fn):
        pl.semaphore_signal(barrier, inc=1, device_id={"fsdp": lax.rem(f + d, fn)}, device_id_type=MESH)
    pl.semaphore_wait(barrier, n - 1 + fn - 1)

    def remote(src, dst, send, recv, **device):
        return pltpu.make_async_remote_copy(
            src_ref=src, dst_ref=dst, send_sem=send, recv_sem=recv, device_id=device, device_id_type=MESH)

    patch_copies = [remote(patches, pbuf.at[rows_of(s)], p_send.at[0], p_recv.at[0], seq=partner)]
    for d in range(1, chips):
        patch_copies.append(remote(patches, pbuf.at[rows_of(s)], p_send.at[d], p_recv.at[d], seq=chip_mate(d)))
    for copy in patch_copies[1:] + patch_copies[:1]:
        copy.start()

    far = place // CORES == jnp.where(half == 0, 0, chips - 1)

    def kv_copy(which, d):
        src, dst = ((key, kraw), (value, vbuf))[which]
        to = lax.rem(s + d, n)
        return remote(
            src.at[:, pl.ds(owned(to), width)], dst.at[all_rows_of(s)],
            kv_send.at[which, d], kv_recv.at[which, d], seq=to)

    def start_kv(behind_patches):
        for which in range(2):
            for step in range(1, n):
                d = jnp.where(half == 0, step, n - step)
                to = lax.rem(s + d, n)
                over_pair = jnp.where(to // m == half, to // CORES != s // CORES, far)

                @pl.when(over_pair == behind_patches)
                def _():
                    kv_copy(which, d).start()

    start_kv(False)

    own_rows = pl.ds(pl.multiple_of(f * rows, rows), rows)

    def weight_copies(q):
        return [
            remote(wbuf.at[q, own_rows], wbuf.at[q, own_rows], w_send.at[q, d], w_recv.at[q, d],
                   fsdp=lax.rem(f + d, fn))
            for d in range(1, fn)
        ]

    def dequantize_pair(pair, _):
        for side in range(2):
            q = 2 * pair + side
            pltpu.make_async_copy(
                codes.at[:, pl.ds(chunk_column(q), LANES)], cbuf.at[q], code_sem.at[q]).wait()
            for block in range(rows // BLOCK):
                scale = scales[block, chunk_column(q) // BLOCK]
                piece = cbuf[q, block * BLOCK:(block + 1) * BLOCK, :].astype(jnp.float32) * scale
                at = pl.ds(pl.multiple_of(f * rows + block * BLOCK, BLOCK), BLOCK)
                wbuf[pair, at, side * LANES:(side + 1) * LANES] = piece.astype(jnp.bfloat16)
        for copy in weight_copies(pair):
            copy.start()
        return 0

    lax.fori_loop(0, chunks, dequantize_pair, 0)

    own_copies[0].wait()

    def forward_copy(d):
        at = rows_of(half * m + lax.rem(place + m - d * CORES, m))
        return remote(pbuf.at[at], pbuf.at[at], fw_send.at[d], fw_recv.at[d], seq=partner)

    def patches_out():
        for copy in patch_copies[1:]:
            copy.wait_send()
        start_kv(True)

    def patches_in():
        for d in range(1, chips):
            patch_copies[d].wait_recv()
            forward_copy(d).start()

    @pl.when(far)
    def _():
        patches_out()
        patches_in()

    @pl.when(jnp.logical_not(far))
    def _():
        patches_in()

    patch_copies[0].wait()
    for d in range(1, chips):
        forward_copy(d).wait()

    other = lax.rem(s + m, n)
    half_rows = pl.ds(pl.multiple_of(half * group, group), group)

    def query_copy(k):
        return remote(qsend.at[k], qbuf.at[k, half_rows], q_send.at[k], q_recv.at[k], seq=other)

    def project(pair):
        for copy in weight_copies(pair):
            copy.wait()
        both = jnp.dot(pbuf[...], wbuf[pair], preferred_element_type=jnp.float32)
        for side in range(2):
            q = 2 * pair + side
            normed = column_norm(
                both[:, side * LANES:(side + 1) * LANES], query_gain[:, pl.ds(chunk_column(q), LANES)])
            if q < chunks:
                qsend[q] = normed
                query_copy(q).start()
            else:
                qbuf[q - chunks, half_rows] = normed

    early = (chunks + 2) // 2
    for pair in range(early):
        project(pair)
        if pair == 0:
            pl.when(jnp.logical_not(far))(patches_out)

    own_copies[1].wait()
    for d in range(1, n):
        kv_copy(0, d).wait()

    def key_chunk(k, _):
        at = pl.multiple_of(k * LANES, LANES)
        knorm[k] = column_norm(
            kraw[:, pl.ds(at, LANES)].astype(jnp.float32),
            key_gain[:, pl.ds(pl.multiple_of(owned(s) + at, LANES), LANES)])
        return 0

    lax.fori_loop(0, chunks, key_chunk, 0)

    own_copies[2].wait()
    for d in range(1, n):
        kv_copy(1, d).wait()

    tile = 2 * tokens
    exponent = HDIM ** (-0.5) * math.log2(math.e)

    def out_columns(k):
        return pl.ds(pl.multiple_of(owned(s) + k * LANES, LANES), LANES)

    def out_copy(k, to):
        d = lax.rem(to - s + n, n)
        return remote(obuf.at[k, all_rows_of(to)], out.at[:, out_columns(k)],
                      o_send.at[k, d], o_recv.at[k, d], seq=to)

    def own_out(k):
        return pltpu.make_async_copy(obuf.at[k, all_rows_of(s)], out.at[:, out_columns(k)], own_sem.at[k])

    first = lax.broadcasted_iota(jnp.int32, (tile, LANES), 1) < HDIM
    tiles = n // CORES

    def attend_step(step, _):
        k, i = step // tiles, lax.rem(step, tiles)
        own_side = half * chips + lax.rem(place // CORES + 1 + i, chips)
        chip = jnp.where(i < chips, (1 - half) * chips + i, own_side)
        here = pl.ds(pl.multiple_of(chip * tile, tile), tile)

        @pl.when(i == 0)
        def _():
            query_copy(k).wait()

        values = vbuf[:, pl.ds(pl.multiple_of(k * LANES, LANES), LANES)]
        keys = knorm[k]
        queries = qbuf[k, here]
        results = []
        for mine in (first, jnp.logical_not(first)):
            masked = jnp.where(mine, queries, jnp.zeros_like(queries))
            scores = lax.dot_general(
                masked, keys, (((1,), (1,)), ((), ())), preferred_element_type=jnp.float32)
            largest = jnp.max(scores, axis=-1, keepdims=True)
            probability = jnp.exp2((scores - largest) * exponent)
            normaliser = jnp.sum(probability, axis=-1, keepdims=True)
            blended = jnp.dot(
                probability.astype(jnp.bfloat16), values, preferred_element_type=jnp.float32)
            results.append(blended / normaliser)
        obuf[k, here] = jnp.where(first, results[0], results[1]).astype(jnp.bfloat16)
        for core in range(CORES):
            to = chip * CORES + core

            @pl.when(to != s)
            def _():
                out_copy(k, to).start()

            @pl.when(to == s)
            def _():
                own_out(k).start()

        return 0

    ready = 2 * early - chunks
    lax.fori_loop(0, ready * tiles, attend_step, 0)
    for pair in range(early, chunks):
        project(pair)
    lax.fori_loop(ready * tiles, chunks * tiles, attend_step, 0)

    def finish(k, _):
        own_out(k).wait()
        for d in range(1, n):
            out_copy(k, lax.rem(s + d, n)).wait()
        return 0

    lax.fori_loop(0, chunks, finish, 0)


def fused_per_device(n, fn, patches, weight_codes, block_scales, key_proj, value_proj, query_gain, key_gain):
    _, tokens, features = patches.shape
    rows, columns = weight_codes.shape
    width = columns // n
    chunks = width // LANES
    group = n // 2 * tokens
    bf16 = jnp.bfloat16
    dma = pltpu.SemaphoreType.DMA
    anywhere = pl.BlockSpec(memory_space=pl.ANY)
    vmem = pl.BlockSpec(memory_space=pltpu.VMEM)
    result = pl.pallas_call(
        functools.partial(fused_kernel, n, fn),
        out_shape=jax.ShapeDtypeStruct((tokens, columns), bf16),
        in_specs=[anywhere, anywhere, pl.BlockSpec(memory_space=pltpu.SMEM), anywhere, anywhere, vmem, vmem],
        out_specs=anywhere,
        scratch_shapes=[
            pltpu.VMEM((group, features), bf16),
            pltpu.VMEM((2 * chunks, rows, LANES), jnp.int32),
            pltpu.VMEM((chunks, features, 2 * LANES), bf16),
            pltpu.VMEM((n * tokens, width), bf16),
            pltpu.VMEM((n * tokens, width), bf16),
            pltpu.VMEM((chunks, n * tokens, LANES), bf16),
            pltpu.VMEM((chunks, group, LANES), bf16),
            pltpu.VMEM((chunks, n * tokens, LANES), bf16),
            pltpu.VMEM((chunks, n * tokens, LANES), bf16),
            dma((3,)), dma((2 * chunks,)),
            dma((n,)), dma((n,)), dma((n,)), dma((n,)),
            dma((chunks, fn)), dma((chunks, fn)),
            dma((2, n)), dma((2, n)),
            dma((chunks,)), dma((chunks,)),
            dma((chunks, n)), dma((chunks, n)), dma((chunks,)),
        ],
        compiler_params=pltpu.CompilerParams(
            collective_id=0, has_side_effects=True, vmem_limit_bytes=56 * 1024 * 1024),
    )(
        patches.reshape(tokens, features), weight_codes, block_scales,
        key_proj.reshape(tokens, columns), value_proj.reshape(tokens, columns),
        query_gain.reshape(1, columns), key_gain.reshape(1, columns),
    )
    return result.reshape(1, tokens, columns)


def solution(mesh):
    n, fn = mesh.shape["seq"], mesh.shape["fsdp"]
    specs = (
        P("fsdp", "seq", None), P("fsdp", None), P("fsdp", None),
        P("fsdp", "seq", None), P("fsdp", "seq", None), P(), P(),
    )

    def whole(*arrays):
        patches, weight_codes = arrays[:2]
        fits = patches.shape[0] == fn and weight_codes.shape[1] % (n * LANES) == 0 and n % (2 * CORES) == 0
        body = functools.partial(fused_per_device, n, fn) if fits else per_device
        return jax.shard_map(
            body, mesh=mesh, in_specs=specs, out_specs=P("fsdp", "seq", None), check_vma=False
        )(*arrays)

    return whole
```

```python
import functools
import math
import jax
import jax.numpy as jnp
from jax import lax
from jax.experimental import pallas as pl
from jax.experimental.pallas import tpu as pltpu
from jax.sharding import PartitionSpec as P

HEADS = 48
HDIM = 64
BLOCK = 128


NORM_FLOOR = 0.25


def head_norm(projected, gain_row):
    shaped = projected.reshape(projected.shape[:-1] + (HEADS, HDIM))
    average = jnp.mean(shaped, axis=-1, keepdims=True)
    centred = shaped - average
    spread = jnp.mean(centred * centred, axis=-1, keepdims=True)
    normed = centred * lax.rsqrt(spread + NORM_FLOOR) * gain_row.reshape(HEADS, HDIM)
    return normed.astype(jnp.bfloat16)


def dequantize(weight_codes, block_scales):
    row_count, column_count = weight_codes.shape
    blocked = weight_codes.astype(jnp.float32).reshape(
        row_count // BLOCK, BLOCK, column_count // BLOCK, BLOCK
    )
    return (
        (blocked * block_scales[:, None, :, None])
        .reshape(row_count, column_count)
        .astype(jnp.bfloat16)
    )


def start_of(query_view):
    image_count, token_count, head_count = (
        query_view.shape[0],
        query_view.shape[1],
        query_view.shape[2],
    )
    return (
        jnp.full((image_count, token_count, head_count), -1e30, jnp.float32),
        jnp.zeros((image_count, token_count, head_count), jnp.float32),
        jnp.zeros(query_view.shape, jnp.float32),
    )


def attend_block(query_view, state_now, key_view, value_view):
    running_max, running_sum, weighted = state_now
    scores = jnp.einsum(
        "ithd,ishd->iths", query_view, key_view, preferred_element_type=jnp.float32
    ) * HDIM ** (-0.5)
    newest = jnp.maximum(running_max, jnp.max(scores, axis=-1))
    probability = jnp.exp(scores - newest[..., None])
    running_sum = jnp.sum(probability, axis=-1)
    blended = jnp.einsum(
        "iths,ishd->ithd",
        probability.astype(jnp.bfloat16),
        value_view,
        preferred_element_type=jnp.float32,
    )
    weighted = blended
    return (newest, running_sum, weighted)


def per_device(patches, weight_codes, block_scales, key_proj, value_proj, query_gain, key_gain):
    image_count, token_count, feature_count = patches.shape
    flat_rows = patches.reshape(image_count * token_count, feature_count)
    key_norm = head_norm(key_proj.astype(jnp.float32), key_gain)
    value_view = value_proj.reshape(image_count, token_count, HEADS, HDIM)
    local_weight = dequantize(weight_codes, block_scales)
    group_rows = lax.all_to_all(flat_rows, "fsdp", split_axis=1, concat_axis=0, tiled=True)
    queries = lax.psum_scatter(
        jnp.dot(group_rows, local_weight, preferred_element_type=jnp.float32),
        "fsdp",
        scatter_dimension=0,
        tiled=True,
    )
    query_view = head_norm(queries, query_gain).reshape(image_count, token_count, HEADS, HDIM)
    finished = attend_block(
        query_view,
        start_of(query_view),
        lax.all_gather(key_norm, "seq", axis=1, tiled=True),
        lax.all_gather(value_view, "seq", axis=1, tiled=True),
    )
    attended = finished[2] / finished[1][..., None]
    return attended.reshape(image_count, token_count, HEADS * HDIM).astype(jnp.bfloat16)


MESH = pl.DeviceIdType.MESH
LANES = 128
CORES = 2
GRID = 2


def column_norm(values, gain_row):
    lane = lambda axis: lax.broadcasted_iota(jnp.int32, (LANES, LANES), axis) < HDIM
    spread_out = jnp.where(lane(0) == lane(1), 1.0 / HDIM, 0.0).astype(jnp.bfloat16)
    spread_out = jnp.concatenate([spread_out, spread_out], axis=0)

    def mean_of(t):
        high = t.astype(jnp.bfloat16)
        low = (t - high.astype(jnp.float32)).astype(jnp.bfloat16)
        return jnp.dot(jnp.concatenate([high, low], axis=1), spread_out, preferred_element_type=jnp.float32)

    centred = values - mean_of(values)
    normed = centred * lax.rsqrt(mean_of(centred * centred) + NORM_FLOOR) * gain_row
    return normed.astype(jnp.bfloat16)


def fused_kernel(
    n, fn, patches, codes, scales, key, value, query_gain, key_gain, out,
    pbuf, cbuf, wbuf, kraw, vbuf, knorm, qsend, qbuf, obuf,
    local_sem, code_sem, p_send, p_recv, fw_send, fw_recv, w_send, w_recv,
    kv_send, kv_recv, q_send, q_recv, o_send, o_recv, own_sem,
):
    s, f = lax.axis_index("seq"), lax.axis_index("fsdp")
    m = n // 2
    half, place = s // m, lax.rem(s, m)
    tokens = patches.shape[0]
    rows, columns = codes.shape
    width = columns // n
    chunks = width // LANES
    group = m * tokens
    chips = m // CORES
    partner = s + 1 - 2 * lax.rem(s, CORES)

    def chip_mate(d):
        return half * m + lax.rem(place + d * CORES, m)

    def rows_of(device):
        return pl.ds(pl.multiple_of(lax.rem(device, m) * tokens, tokens), tokens)

    def all_rows_of(device):
        return pl.ds(pl.multiple_of(device * tokens, tokens), tokens)

    def owned(device):
        return pl.multiple_of((lax.rem(device, m) * 2 + device // m) * width, LANES)

    def chunk_column(q):
        side = jnp.where(q < chunks, 1 - half, half)
        return pl.multiple_of((place * 2 + side) * width + lax.rem(q, chunks) * LANES, LANES)

    code_copies = []
    for q in range(2 * chunks):
        code_copies.append(pltpu.make_async_copy(
            codes.at[:, pl.ds(chunk_column(q), LANES)], cbuf.at[q], code_sem.at[q]))
        code_copies[-1].start()
    own_copies = [
        pltpu.make_async_copy(patches, pbuf.at[rows_of(s)], local_sem.at[0]),
        pltpu.make_async_copy(key.at[:, pl.ds(owned(s), width)], kraw.at[all_rows_of(s)], local_sem.at[1]),
        pltpu.make_async_copy(value.at[:, pl.ds(owned(s), width)], vbuf.at[all_rows_of(s)], local_sem.at[2]),
    ]
    for copy in own_copies:
        copy.start()

    barrier = pltpu.get_barrier_semaphore()
    for d in range(1, n):
        pl.semaphore_signal(barrier, inc=1, device_id={"seq": lax.rem(s + d, n)}, device_id_type=MESH)
    for d in range(1, fn):
        pl.semaphore_signal(barrier, inc=1, device_id={"fsdp": lax.rem(f + d, fn)}, device_id_type=MESH)
    pl.semaphore_wait(barrier, n - 1 + fn - 1)

    def remote(src, dst, send, recv, **device):
        return pltpu.make_async_remote_copy(
            src_ref=src, dst_ref=dst, send_sem=send, recv_sem=recv, device_id=device, device_id_type=MESH)

    patch_copies = [remote(patches, pbuf.at[rows_of(s)], p_send.at[0], p_recv.at[0], seq=partner)]
    for d in range(1, chips):
        patch_copies.append(remote(patches, pbuf.at[rows_of(s)], p_send.at[d], p_recv.at[d], seq=chip_mate(d)))
    for copy in patch_copies[1:] + patch_copies[:1]:
        copy.start()

    far = place // CORES == jnp.where(half == 0, 0, chips - 1)

    def kv_copy(which, d):
        src, dst = ((key, kraw), (value, vbuf))[which]
        to = lax.rem(s + d, n)
        return remote(
            src.at[:, pl.ds(owned(to), width)], dst.at[all_rows_of(s)],
            kv_send.at[which, d], kv_recv.at[which, d], seq=to)

    def start_kv(behind_patches):
        for which in range(2):
            for step in range(1, n):
                d = jnp.where(half == 0, step, n - step)
                to = lax.rem(s + d, n)
                to_far = lax.rem(to, m) // CORES == jnp.where(to // m == 0, 0, chips - 1)
                over_pair = jnp.where(to // m == half, to // CORES != s // CORES, far & to_far)

                @pl.when(over_pair == behind_patches)
                def _():
                    kv_copy(which, d).start()

    start_kv(False)

    row_mate = f + 1 - 2 * lax.rem(f, GRID)
    column_mate = lax.rem(f + GRID, fn)

    def weight_copy(pair, way, start, size, to):
        at = pl.ds(pl.multiple_of(start, size), size)
        return remote(wbuf.at[pair, at], wbuf.at[pair, at], w_send.at[pair, way], w_recv.at[pair, way], fsdp=to)

    def near_copies(pair):
        return [
            weight_copy(pair, 0, f * rows, rows, row_mate),
            weight_copy(pair, 1, f * rows, rows, column_mate),
        ]

    def relay_copies(pair):
        part = rows // 2
        return [
            weight_copy(pair, 2, row_mate * rows, part, column_mate),
            weight_copy(pair, 3, column_mate * rows + part, part, row_mate),
        ]

    def relay(pair):
        for copy in near_copies(pair):
            copy.wait_recv()
        for copy in relay_copies(pair):
            copy.start()

    def relay_early():
        for pair in range(chunks - 1):
            relay(pair)
        for copy in near_copies(chunks - 1):
            copy.start()

    def dequantize_pair(pair, _):
        for side in range(2):
            q = 2 * pair + side
            pltpu.make_async_copy(
                codes.at[:, pl.ds(chunk_column(q), LANES)], cbuf.at[q], code_sem.at[q]).wait()
            for block in range(rows // BLOCK):
                scale = scales[block, chunk_column(q) // BLOCK]
                piece = cbuf[q, block * BLOCK:(block + 1) * BLOCK, :].astype(jnp.float32) * scale
                at = pl.ds(pl.multiple_of(f * rows + block * BLOCK, BLOCK), BLOCK)
                wbuf[pair, at, side * LANES:(side + 1) * LANES] = piece.astype(jnp.bfloat16)

        @pl.when(pair < chunks - 1)
        def _():
            for copy in near_copies(pair):
                copy.start()

        return 0

    lax.fori_loop(0, chunks, dequantize_pair, 0)

    own_copies[0].wait()

    def forward_copy(d):
        at = rows_of(half * m + lax.rem(place + m - d * CORES, m))
        return remote(pbuf.at[at], pbuf.at[at], fw_send.at[d], fw_recv.at[d], seq=partner)

    def patches_out():
        for copy in patch_copies[1:]:
            copy.wait_send()
        start_kv(True)

    def patches_in():
        for d in range(1, chips):
            patch_copies[d].wait_recv()
            forward_copy(d).start()

    @pl.when(far)
    def _():
        patches_out()
        relay_early()
        patches_in()

    @pl.when(jnp.logical_not(far))
    def _():
        patches_in()
        relay_early()

    patch_copies[0].wait()
    for d in range(1, chips):
        forward_copy(d).wait()

    other = lax.rem(s + m, n)
    half_rows = pl.ds(pl.multiple_of(half * group, group), group)

    def query_copy(k):
        return remote(qsend.at[k], qbuf.at[k, half_rows], q_send.at[k], q_recv.at[k], seq=other)

    def project(pair):
        for copy in near_copies(pair):
            copy.wait_send()
        for copy in relay_copies(pair):
            copy.wait()
        both = jnp.dot(pbuf[...], wbuf[pair], preferred_element_type=jnp.float32)
        for side in range(2):
            q = 2 * pair + side
            normed = column_norm(
                both[:, side * LANES:(side + 1) * LANES], query_gain[:, pl.ds(chunk_column(q), LANES)])
            if q < chunks:
                qsend[q] = normed
                query_copy(q).start()
            else:
                qbuf[q - chunks, half_rows] = normed

    early = (chunks + 2) // 2
    for pair in range(early):
        project(pair)
        if pair == 0:
            pl.when(jnp.logical_not(far))(patches_out)
    relay(chunks - 1)

    own_copies[1].wait()
    for d in range(1, n):
        kv_copy(0, d).wait()

    def key_chunk(k, _):
        at = pl.multiple_of(k * LANES, LANES)
        knorm[k] = column_norm(
            kraw[:, pl.ds(at, LANES)].astype(jnp.float32),
            key_gain[:, pl.ds(pl.multiple_of(owned(s) + at, LANES), LANES)])
        return 0

    lax.fori_loop(0, chunks, key_chunk, 0)

    own_copies[2].wait()
    for d in range(1, n):
        kv_copy(1, d).wait()

    tile = 2 * tokens
    exponent = HDIM ** (-0.5) * math.log2(math.e)

    def out_columns(k):
        return pl.ds(pl.multiple_of(owned(s) + k * LANES, LANES), LANES)

    def out_copy(k, to):
        d = lax.rem(to - s + n, n)
        return remote(obuf.at[k, all_rows_of(to)], out.at[:, out_columns(k)],
                      o_send.at[k, d], o_recv.at[k, d], seq=to)

    def own_out(k):
        return pltpu.make_async_copy(obuf.at[k, all_rows_of(s)], out.at[:, out_columns(k)], own_sem.at[k])

    first = lax.broadcasted_iota(jnp.int32, (tile, LANES), 1) < HDIM
    tiles = n // CORES

    def attend_step(step, _):
        k, i = step // tiles, lax.rem(step, tiles)
        own_side = half * chips + lax.rem(place // CORES + 1 + i, chips)
        chip = jnp.where(i < chips, (1 - half) * chips + i, own_side)
        here = pl.ds(pl.multiple_of(chip * tile, tile), tile)

        @pl.when(i == 0)
        def _():
            query_copy(k).wait()

        values = vbuf[:, pl.ds(pl.multiple_of(k * LANES, LANES), LANES)]
        keys = knorm[k]
        queries = qbuf[k, here]
        results = []
        for mine in (first, jnp.logical_not(first)):
            masked = jnp.where(mine, queries, jnp.zeros_like(queries))
            scores = lax.dot_general(
                masked, keys, (((1,), (1,)), ((), ())), preferred_element_type=jnp.float32)
            largest = jnp.max(scores, axis=-1, keepdims=True)
            probability = jnp.exp2((scores - largest) * exponent)
            normaliser = jnp.sum(probability, axis=-1, keepdims=True)
            blended = jnp.dot(
                probability.astype(jnp.bfloat16), values, preferred_element_type=jnp.float32)
            results.append(blended / normaliser)
        obuf[k, here] = jnp.where(first, results[0], results[1]).astype(jnp.bfloat16)
        for core in range(CORES):
            to = chip * CORES + core

            @pl.when(to != s)
            def _():
                out_copy(k, to).start()

            @pl.when(to == s)
            def _():
                own_out(k).start()

        return 0

    ready = 2 * early - chunks
    lax.fori_loop(0, ready * tiles, attend_step, 0)
    for pair in range(early, chunks):
        project(pair)
    lax.fori_loop(ready * tiles, chunks * tiles, attend_step, 0)

    def finish(k, _):
        own_out(k).wait()
        for d in range(1, n):
            out_copy(k, lax.rem(s + d, n)).wait()
        return 0

    lax.fori_loop(0, chunks, finish, 0)


def fused_per_device(n, fn, patches, weight_codes, block_scales, key_proj, value_proj, query_gain, key_gain):
    _, tokens, features = patches.shape
    rows, columns = weight_codes.shape
    width = columns // n
    chunks = width // LANES
    group = n // 2 * tokens
    bf16 = jnp.bfloat16
    dma = pltpu.SemaphoreType.DMA
    anywhere = pl.BlockSpec(memory_space=pl.ANY)
    vmem = pl.BlockSpec(memory_space=pltpu.VMEM)
    result = pl.pallas_call(
        functools.partial(fused_kernel, n, fn),
        out_shape=pltpu.VMEM((tokens, columns), bf16),
        in_specs=[anywhere, anywhere, pl.BlockSpec(memory_space=pltpu.SMEM), anywhere, anywhere, vmem, vmem],
        out_specs=vmem,
        scratch_shapes=[
            pltpu.VMEM((group, features), bf16),
            pltpu.VMEM((2 * chunks, rows, LANES), jnp.int32),
            pltpu.VMEM((chunks, features, 2 * LANES), bf16),
            pltpu.VMEM((n * tokens, width), bf16),
            pltpu.VMEM((n * tokens, width), bf16),
            pltpu.VMEM((chunks, n * tokens, LANES), bf16),
            pltpu.VMEM((chunks, group, LANES), bf16),
            pltpu.VMEM((chunks, n * tokens, LANES), bf16),
            pltpu.VMEM((chunks, n * tokens, LANES), bf16),
            dma((3,)), dma((2 * chunks,)),
            dma((n,)), dma((n,)), dma((n,)), dma((n,)),
            dma((chunks, fn)), dma((chunks, fn)),
            dma((2, n)), dma((2, n)),
            dma((chunks,)), dma((chunks,)),
            dma((chunks, n)), dma((chunks, n)), dma((chunks,)),
        ],
        compiler_params=pltpu.CompilerParams(
            collective_id=0, has_side_effects=True, vmem_limit_bytes=56 * 1024 * 1024),
    )(
        patches.reshape(tokens, features), weight_codes, block_scales,
        key_proj.reshape(tokens, columns), value_proj.reshape(tokens, columns),
        query_gain.reshape(1, columns), key_gain.reshape(1, columns),
    )
    return result.reshape(1, tokens, columns)


def solution(mesh):
    n, fn = mesh.shape["seq"], mesh.shape["fsdp"]
    specs = (
        P("fsdp", "seq", None), P("fsdp", None), P("fsdp", None),
        P("fsdp", "seq", None), P("fsdp", "seq", None), P(), P(),
    )

    def whole(*arrays):
        patches, weight_codes = arrays[:2]
        fits = patches.shape[0] == fn == GRID * GRID and weight_codes.shape[1] % (n * LANES) == 0 and n % (2 * CORES) == 0
        body = functools.partial(fused_per_device, n, fn) if fits else per_device
        return jax.shard_map(
            body, mesh=mesh, in_specs=specs, out_specs=P("fsdp", "seq", None), check_vma=False
        )(*arrays)

    return whole
```
